8 devices in a mesh: data: 2 (over z, y), expert: 4 (over x, core).
Axes of the slice: x: 2, y: 2, z: 1, core: 2. Of those that a mesh axis runs over, the one named last changes fastest.
Arguments:
- x_tok: bfloat16 [16384, 2304], P(('data', 'expert')), parts along dimension 0
- topk_idx: int32 [16384, 2], P(('data', 'expert')), parts along dimension 0
- topk_w: float32 [16384, 2], P(('data', 'expert')), parts along dimension 0
- w_up: bfloat16 [8, 2304, 5760], P('expert')
- w_down: bfloat16 [8, 5760, 2304], P('expert')
Outputs:
- output: bfloat16 [16384, 2304], P(('data', 'expert')), parts along dimension 0
There are 2 independent parts. The reference program is written for one: setup_inputs(seed, part) draws one part's arguments, and reference() takes and returns one part's arrays. A program takes and returns all parts, laid end to end along the dimension named above; an argument that names none is the same for every part.
All inputs are finite; a program needn't handle non-finite values.
Results may differ from the reference program's by a relative error of at most 0.001.
Values are sent between devices in bfloat16 or wider.
A program may use at most 1 GiB of HBM per device.

```python
import jax
import jax.numpy as jnp
from jax import lax

D_MODEL = 2304
D_FF = 5760
EXPERTS = 8
TOP_K = 2
TOK_DEV = 2048
GROUP_SIZE = 4
HOT_MUL = min(4, EXPERTS // TOP_K)
SLOT_CAP = HOT_MUL * TOK_DEV * TOP_K // EXPERTS
NUM_HOT = max(1, EXPERTS // 32)
TOKENS = GROUP_SIZE * TOK_DEV


def draw_routing(key):
    hot_key, dev_key = jax.random.split(key)
    exp_perm = jax.random.permutation(hot_key, EXPERTS)
    n_cold = EXPERTS - NUM_HOT
    cold_total = TOK_DEV * TOP_K - NUM_HOT * SLOT_CAP
    base_count = cold_total // n_cold
    extra_count = cold_total - base_count * n_cold

    def one_device(dev_seed):
        shift_key, order_key, perm_key = jax.random.split(dev_seed, 3)
        shifts = jax.random.randint(shift_key, (n_cold // 2,), 0, base_count // 2 + 1)
        count_shift = jnp.concatenate([jnp.stack([shifts, -shifts], axis=1).reshape(-1), jnp.zeros((n_cold % 2,), jnp.int32)])
        cold_counts = base_count + (jnp.arange(n_cold) < extra_count).astype(jnp.int32) + count_shift
        counts = jnp.concatenate([jnp.full((NUM_HOT,), SLOT_CAP, jnp.int32), cold_counts])
        visit_order = jax.random.permutation(order_key, EXPERTS)
        run_ends = jnp.cumsum(counts[visit_order])
        run_index = jnp.searchsorted(run_ends, jnp.arange(TOK_DEV * TOP_K), side='right')
        pair_seq = exp_perm[visit_order][run_index]
        choice = pair_seq.reshape(TOP_K, TOK_DEV).T
        return choice[jax.random.permutation(perm_key, TOK_DEV)]

    dev_keys = jax.random.split(dev_key, GROUP_SIZE)
    return jax.vmap(one_device)(dev_keys).reshape(TOKENS, TOP_K).astype(jnp.int32)


def setup_inputs(seed: int = 0, part: int = 0) -> dict:
    part_key = jax.random.fold_in(jax.random.key(seed), part)
    route_key, gate_key, tok_key = jax.random.split(part_key, 3)
    up_key, down_key = jax.random.split(jax.random.key(seed + 1))
    x_tok = jax.random.normal(tok_key, (TOKENS, D_MODEL), jnp.float32).astype(jnp.bfloat16)
    topk_idx = draw_routing(route_key)
    topk_w = jax.random.uniform(gate_key, (TOKENS, TOP_K), jnp.float32, 0.1, 1.0)
    w_up = (jax.random.normal(up_key, (EXPERTS, D_MODEL, D_FF), jnp.float32) * D_MODEL ** -0.5).astype(jnp.bfloat16)
    w_down = (jax.random.normal(down_key, (EXPERTS, D_FF, D_MODEL), jnp.float32) * D_FF ** -0.5).astype(jnp.bfloat16)
    return {'x_tok': x_tok, 'topk_idx': topk_idx, 'topk_w': topk_w, 'w_up': w_up, 'w_down': w_down}


def reference(x_tok, topk_idx, topk_w, w_up, w_down):
    pair_exp = topk_idx.reshape(-1)
    n_pairs = TOKENS * TOP_K
    group_cap = GROUP_SIZE * SLOT_CAP
    sort_order = jnp.argsort(pair_exp, stable=True)
    pair_rank = jnp.argsort(sort_order, stable=True)
    counts = jnp.bincount(pair_exp, length=EXPERTS)
    starts = jnp.cumsum(counts) - counts
    slot_src = jnp.minimum(starts[:, None] + jnp.arange(group_cap)[None, :], n_pairs - 1)
    slot_tok = sort_order[slot_src] // TOP_K

    def expert_rows(operands):
        tok_ids, up_mat, down_mat = operands
        tok_rows = x_tok[tok_ids]
        hidden = jnp.dot(tok_rows, up_mat, preferred_element_type=jnp.float32)
        hidden = jax.nn.gelu(hidden, approximate=True).astype(jnp.bfloat16)
        return jnp.dot(hidden, down_mat, preferred_element_type=jnp.float32).astype(jnp.bfloat16)

    slot_out = lax.map(expert_rows, (slot_tok, w_up, w_down)).reshape(EXPERTS * group_cap, D_MODEL)
    pair_slot = pair_exp * group_cap + pair_rank - starts[pair_exp]
    pair_out = slot_out[pair_slot].reshape(TOKENS, TOP_K, D_MODEL)
    y_tok = jnp.sum(topk_w[:, :, None] * pair_out.astype(jnp.float32), axis=1)
    return y_tok.astype(jnp.bfloat16)
```

```python
import functools

import jax
import jax.numpy as jnp
from jax import lax
from jax.experimental import pallas as pl
from jax.experimental.pallas import tpu as pltpu
from jax.sharding import PartitionSpec as P


F32, BF16, I32 = jnp.float32, jnp.bfloat16, jnp.int32
HOT_ROWS = 1024
COLD_ROWS = 1024
STEP = 128
GATHER = STEP
UP_COLS = 1920
DOWN_COLS = 768
VMEM_LIMIT = 60 << 20
ANY = pl.BlockSpec(memory_space=pl.ANY)


def params(n):
    return pltpu.CompilerParams(dimension_semantics=("arbitrary",) * n, vmem_limit_bytes=VMEM_LIMIT)


def gelu(v):
    return jax.nn.gelu(v, approximate=True).astype(BF16)


def prep_body(cap, scal, idx_ref, base_ref, pos_ref, cnt_ref):
    hot, own, r1, r2 = scal[0], scal[1], scal[2], scal[3]
    w = 256
    tri = (lax.broadcasted_iota(I32, (w, w), 0) <= lax.broadcasted_iota(I32, (w, w), 1)).astype(F32)
    base = ((base_ref[...] + STEP - 1) // STEP * STEP)[:, 0:1].astype(F32)
    carry = jnp.zeros((8, 1), F32)
    pos_ref[...] = jnp.full(pos_ref.shape, -1, I32)
    for b in range(idx_ref.shape[1] // w):
        cols = pl.ds(b * w, w)
        c0, c1 = idx_ref[0:1, cols], idx_ref[1:2, cols]
        cold = jnp.where(c0 == hot, c1, c0)
        loc = jnp.where(cold == own, 0, jnp.where(cold == own + 1, 1, jnp.where(cold == r1, 2, jnp.where(cold == r2, 3, -1))))
        mine = (lax.broadcasted_iota(I32, (8, w), 0) == loc).astype(F32)
        upto = jnp.dot(mine, tri, preferred_element_type=F32) + carry
        rank = jnp.sum(mine * (upto + base - 1.0), axis=0, keepdims=True).astype(I32)
        pos_ref[0:1, cols] = jnp.where(loc >= 0, loc * cap + rank, -1)
        carry = upto[:, w - 1:w]
    cnt_ref[...] = jnp.broadcast_to(carry, (8, 128)).astype(I32)


def prep(scal, idx8, base, cap):
    vmem = pl.BlockSpec(memory_space=pltpu.VMEM)
    return pl.pallas_call(
        functools.partial(prep_body, cap),
        out_shape=(jax.ShapeDtypeStruct(idx8.shape, I32), jax.ShapeDtypeStruct((8, 128), I32)),
        in_specs=[pl.BlockSpec(memory_space=pltpu.SMEM), vmem, vmem],
        out_specs=(vmem, vmem),
    )(scal, idx8, base)


def gather_body(n_parts, blk, pos_ref, *refs):
    parts, out_ref = refs[:n_parts], refs[-1]
    i = pl.program_id(0)

    @pl.when(i < blk[pl.num_programs(0)])
    def _():
        total, start = None, 0
        for part in parts:
            width = part.shape[0]
            slot = blk[i] * GATHER + lax.broadcasted_iota(I32, (GATHER, width), 0)
            pick = (pos_ref[0:1, start:start + width] == slot).astype(F32).astype(BF16)
            term = jnp.dot(pick, part[...], preferred_element_type=F32)
            total = term if total is None else total + term
            start += width
        out_ref[...] = total.astype(BF16)


def gather(blk, pos, parts, slots, prev, dep):
    d = parts[0].shape[1]
    alias = prev is not None
    return pl.pallas_call(
        functools.partial(gather_body, len(parts)),
        out_shape=jax.ShapeDtypeStruct((slots, d), BF16),
        grid_spec=pltpu.PrefetchScalarGridSpec(
            num_scalar_prefetch=1, grid=(blk.shape[0] - 1,),
            in_specs=[pl.BlockSpec(pos.shape, lambda i, b: (0, 0))]
            + [pl.BlockSpec(p.shape, lambda i, b: (0, 0)) for p in parts] + [ANY] * (1 + alias),
            out_specs=pl.BlockSpec((GATHER, d), lambda i, b: (b[i], 0))),
        input_output_aliases={3 + len(parts): 0} if alias else {},
        compiler_params=params(1),
    )(blk, pos, *parts, dep, *([prev] if alias else []))


def ffn_body(n_sets, rb, hot, x_ref, *refs):
    metas, ups, downs = refs[:n_sets], refs[n_sets:2 * n_sets], refs[2 * n_sets:3 * n_sets]
    out_ref, hid_ref = refs[-2:]
    d, ff = ups[0].shape[1:]

    def for_rows(meta, i, run):
        if hot:
            lax.fori_loop(0, rb // 512, lambda r, c: (run(r * 512, 512), c)[1], 0)
            return
        steps = meta[2, i]
        lax.fori_loop(0, steps // 2, lambda r, c: (run(r * 256, 256), c)[1], 0)

        @pl.when(steps % 2 == 1)
        def _():
            run((steps - 1) * STEP, STEP)

    for meta, up, down in zip(metas, ups, downs):
        n = meta[3, 0]

        def up_step(step, x, w, h, meta=meta):
            def run(r, m):
                rows = pl.ds(pl.multiple_of(r, m), m)
                h[rows, :] = gelu(jnp.dot(x[rows, :], w[0], preferred_element_type=F32))

            for_rows(meta, step.index[0], run)

        def down_step(step, h, w, o, meta=meta):
            if not hot:
                o[...] = jnp.zeros_like(o)

            def run(r, m):
                rows = pl.ds(pl.multiple_of(r, m), m)
                o[rows, :] = jnp.dot(h[rows, :], w[0], preferred_element_type=F32).astype(BF16)

            for_rows(meta, step.index[0], run)

        @pl.when(n > 0)
        def _(meta=meta, up=up, down=down, up_step=up_step, down_step=down_step, n=n):
            pltpu.emit_pipeline(
                up_step, grid=(n, ff // UP_COLS),
                in_specs=[pl.BlockSpec((rb, d), lambda i, f: (meta[0, i], 0)),
                          pl.BlockSpec((1, d, UP_COLS), lambda i, f: (meta[1, i], 0, f))],
                out_specs=[pl.BlockSpec((rb, UP_COLS), lambda i, f: (i, f))],
                _explicit_indices=True,
            )(x_ref, up, hid_ref)
            pltpu.emit_pipeline(
                down_step, grid=(n, d // DOWN_COLS),
                in_specs=[pl.BlockSpec((rb, ff), lambda i, c: (i, 0)),
                          pl.BlockSpec((1, ff, DOWN_COLS), lambda i, c: (meta[1, i], 0, c))],
                out_specs=[pl.BlockSpec((rb, DOWN_COLS), lambda i, c: (meta[0, i], c))],
                _explicit_indices=True,
            )(hid_ref, down, out_ref)


def ffn(sets, x, dep, prev, rb, hot, out_rows):
    n = len(sets)
    metas, ups, downs = zip(*sets)
    d, ff = ups[0].shape[1:]
    max_items = max(m.shape[1] for m in metas)
    alias = prev is not None
    out, _ = pl.pallas_call(
        functools.partial(ffn_body, n, rb, hot),
        out_shape=(jax.ShapeDtypeStruct((out_rows, d), BF16), jax.ShapeDtypeStruct((max_items * rb, ff), BF16)),
        in_specs=[ANY] + [pl.BlockSpec(memory_space=pltpu.SMEM)] * n + [ANY] * (2 * n + 1 + alias),
        out_specs=(ANY, ANY),
        input_output_aliases={3 * n + 2: 0} if alias else {},
        compiler_params=pltpu.CompilerParams(vmem_limit_bytes=VMEM_LIMIT),
    )(x, *metas, *ups, *downs, dep, *([prev] if alias else []))
    return out


def after_body(value, dep, out):
    out[0] = value[0]


def after(value, dep):
    smem = pl.BlockSpec(memory_space=pltpu.SMEM)
    return pl.pallas_call(after_body, out_shape=jax.ShapeDtypeStruct((1,), I32), in_specs=[smem, ANY], out_specs=smem)(
        value.astype(I32)[None], dep)[0]


def join_body(local, blk, scal, pos_ref, gate_ref, hot_ref, cold_ref, out_ref, acc):
    k = pl.program_id(1)
    t = pos_ref.shape[0]

    @pl.when(k == 0)
    def _():
        acc[...] = jnp.zeros_like(acc)

    @pl.when(k < blk[pl.num_programs(1)])
    def _():
        slot = blk[k] * GATHER + lax.broadcasted_iota(I32, (t, GATHER), 1)
        pick = (pos_ref[:, 0:1] == slot).astype(F32).astype(BF16)
        acc[...] += jnp.dot(pick, cold_ref[...], preferred_element_type=F32)

    @pl.when(k == pl.num_programs(1) - 1)
    def _():
        for r in range(0, t, 256):
            rows = slice(r, r + 256)
            here = jnp.broadcast_to(pos_ref[rows, 0:1], (256, acc.shape[1])) >= 0
            g_hot, g_cold = gate_ref[rows, 0:1], gate_ref[rows, 1:2]
            o_hot, o_cold = hot_ref[rows, :].astype(F32), acc[rows, :]

            @pl.when(scal[0] == 1)
            def _():
                if local:
                    out_ref[rows, :] = g_hot * o_hot + jnp.where(here, g_cold * o_cold, 0.0)
                else:
                    out_ref[rows, :] = jnp.where(here, g_hot * o_hot + g_cold * o_cold, o_hot).astype(BF16)

            @pl.when(scal[0] == 0)
            def _():
                if local:
                    out_ref[rows, :] = jnp.where(here, g_cold * o_cold, 0.0)
                else:
                    out_ref[rows, :] = o_cold.astype(BF16)


def join(blk, scal, pos_col, gates, o_hot, o_cold, local, first, rows):
    d = o_hot.shape[1]
    tb = 1024
    return pl.pallas_call(
        functools.partial(join_body, local),
        out_shape=jax.ShapeDtypeStruct((rows, d), F32 if local else BF16),
        grid_spec=pltpu.PrefetchScalarGridSpec(
            num_scalar_prefetch=2, grid=(rows // tb, blk.shape[0] - 1),
            in_specs=[pl.BlockSpec((tb, 1), lambda i, k, b, s: (i + first, 0)),
                      pl.BlockSpec((tb, 2), lambda i, k, b, s: (i + first, 0)),
                      pl.BlockSpec((tb, d), lambda i, k, b, s: (i, 0)),
                      pl.BlockSpec((GATHER, d), lambda i, k, b, s: (b[k], 0))],
            out_specs=pl.BlockSpec((tb, d), lambda i, k, b, s: (i, 0)),
            scratch_shapes=[pltpu.VMEM((tb, d), F32)]),
        compiler_params=params(2),
    )(blk, scal, pos_col, gates, o_hot, o_cold)


def final_body(part_ref, gate_ref, back_ref, prev_ref, out_ref):
    out_ref[...] = (part_ref[...] + gate_ref[...] * back_ref[...].astype(F32)).astype(BF16)


def final(part, gate, back, prev, half):
    rows, d = part.shape
    tb = 256
    n = rows // 2 // tb
    return pl.pallas_call(
        final_body,
        out_shape=jax.ShapeDtypeStruct((rows, d), BF16),
        grid=(n,),
        in_specs=[pl.BlockSpec((tb, d), lambda i: (i + half * n, 0)), pl.BlockSpec((tb, 1), lambda i: (i + half * n, 0)),
                  pl.BlockSpec((tb, d), lambda i: (i, 0)), ANY],
        out_specs=pl.BlockSpec((tb, d), lambda i: (i + half * n, 0)),
        input_output_aliases={3: 0} if prev is not None else {},
        compiler_params=params(1),
    )(part, gate, back, prev if prev is not None else back)


def cold_items(steps, locs, cap):
    per = COLD_ROWS // STEP
    n = [(steps[l] + per - 1) // per for l in locs]
    i = jnp.arange(cap // COLD_ROWS + len(locs), dtype=I32)
    block, exp, left = locs[0] * (cap // COLD_ROWS) + i, jnp.zeros_like(i), steps[locs[0]] - i * per
    if len(locs) == 2:
        second = i >= n[0]
        j = i - n[0]
        block = jnp.where(second, locs[1] * (cap // COLD_ROWS) + j, block)
        exp = second.astype(I32)
        left = jnp.where(second, steps[locs[1]] - j * per, left)
    return jnp.stack([jnp.clip(block, 0, 4 * cap // COLD_ROWS - 1), exp, jnp.clip(left, 1, per), jnp.full_like(i, sum(n))])


def gather_blocks(n, first, cap, tokens):
    i = jnp.arange(tokens // GATHER + 4, dtype=I32)
    i = jnp.minimum(i, sum(n) - 1)
    blk, start = jnp.zeros_like(i), 0
    for l in range(4):
        blk = jnp.where(i >= start, l * (cap // GATHER) + first[l] + i - start, blk)
        start = start + n[l]
    return jnp.concatenate([jnp.clip(blk, 0, 4 * cap // GATHER - 1), jnp.full((1,), start, I32)])


def solution(mesh):
    group = mesh.shape['expert']
    n_exp = 2 * group
    sib = [(i, i ^ 1) for i in range(group)]
    far = [(i, i ^ 2) for i in range(group)]

    def send(v, pairs):
        return lax.ppermute(v, 'expert', pairs)

    def layer(x, idx, gate, up, down):
        tokens, _ = x.shape
        half = tokens // 2
        cap = 2 * tokens
        me = lax.axis_index('expert')
        p_idx = send(idx, far)
        p_gate = send(gate, far)

        taken = [jnp.sum((idx == k).astype(I32)) == tokens for k in range(n_exp)]
        hot = sum(jnp.where(t, k, 0) for k, t in enumerate(taken)).astype(I32)
        owner = hot // 2
        sel = jnp.where(owner == me, hot % 2, 0)
        peer = me ^ 1
        p_sel = jnp.where(owner == peer, hot % 2, 0)
        ids = jnp.stack([hot, 2 * me, 2 * peer + p_sel, 2 * peer + 1 - p_sel]).astype(I32)
        hot_here = owner // 2 == me // 2
        flag = hot_here.astype(I32)[None]

        far1 = send(x[:half], far)
        far2 = send(x[half:], far)
        sel_1 = after(sel, idx)
        up1 = lax.dynamic_slice_in_dim(up, sel_1, 1, 0)
        down1 = lax.dynamic_slice_in_dim(down, after(sel_1, up1), 1, 0)
        other = after(1 - sel_1, down1)
        up1 = send(up1, sib)
        down1 = send(down1, sib)

        def rows8(i):
            return jnp.concatenate([i.T, jnp.full((6, tokens), -1, I32)], axis=0)

        pos_o, cnt_o = prep(ids, rows8(idx), jnp.zeros((8, 128), I32), cap)
        pos_p, cnt_p = prep(ids, rows8(p_idx), cnt_o, cap)
        n_o = [(cnt_o[l, 0] + STEP - 1) // STEP for l in range(4)]
        n_p = [(cnt_p[l, 0] + STEP - 1) // STEP for l in range(4)]
        n_all = [a + b for a, b in zip(n_o, n_p)]
        blk_o = gather_blocks(n_o, [0] * 4, cap, tokens)
        blk_p = gather_blocks(n_p, n_o, cap, tokens)
        col_o, col_p = pos_o[0][:, None], pos_p[0][:, None]

        rows_o = gather(blk_o, pos_o, (x,), 4 * cap, None, pos_o)
        up2 = send(lax.dynamic_slice_in_dim(up, other, 1, 0), sib)
        down2 = send(lax.dynamic_slice_in_dim(down, other, 1, 0), sib)

        def gates(i, g):
            first = i[:, 0:1] == hot
            return jnp.concatenate([jnp.where(first, g[:, 0:1], g[:, 1:2]), jnp.where(first, g[:, 1:2], g[:, 0:1])], axis=1)

        g_o, g_p = gates(idx, gate), gates(p_idx, p_gate)
        here = col_o >= 0
        g_back = jnp.where(hot_here, jnp.where(here, 0.0, g_o[:, 1:2]), jnp.where(here, g_o[:, 0:1], 1.0))
        own_hot, got_hot = (owner == me).astype(I32), (owner == peer).astype(I32)

        def run_hot(xs, first, n, sets, dep, prev):
            i = jnp.arange(n, dtype=I32)
            sets = [(jnp.stack([i + first, jnp.full_like(i, exp), i, jnp.full_like(i, n * on)]), u, dn) for exp, on, u, dn in sets]
            return ffn(sets, xs, dep, prev, HOT_ROWS, True, xs.shape[0])

        hot_own, hot_got = (hot % 2, own_hot, up, down), (0, got_hot, up1, down1)
        hot_o = run_hot(x, 0, 2, [hot_own], rows_o, None)
        hot_1 = run_hot(far1, 0, 1, [hot_own, hot_got], hot_o, None)
        hot_o = run_hot(x, 0, 1, [hot_got], hot_1, hot_o)
        rows = gather(blk_p, pos_p, (far1, far2), 4 * cap, rows_o, hot_o)
        sets = [(cold_items(n_all, (0, 1), cap), up, down), (cold_items(n_all, (2,), cap), up1, down1),
                (cold_items(n_all, (3,), cap), up2, down2)]
        cold = ffn(sets, rows, rows, None, COLD_ROWS, False, 4 * cap)
        out_1 = join(blk_p, flag, col_p, g_p, hot_1, cold, False, 0, half)
        back_1 = send(out_1, far)
        hot_2 = run_hot(far2, 0, 1, [hot_own, hot_got], out_1, None)
        out_2 = join(blk_p, flag, col_p, g_p, hot_2, cold, False, 1, half)
        back_2 = send(out_2, far)
        hot_o = run_hot(x, 1, 1, [hot_got], out_2, hot_o)
        part = join(blk_o, flag, col_o, g_o, hot_o, cold, True, 0, tokens)
        y = final(part, g_back, back_1, None, 0)
        return final(part, g_back, back_2, y, 1)

    tok_spec = P(('data', 'expert'), None)
    w_spec = P('expert', None, None)
    return jax.shard_map(layer, mesh=mesh, in_specs=(tok_spec, tok_spec, tok_spec, w_spec, w_spec), out_specs=tok_spec, check_vma=False)
```

```python
import functools

import jax
import jax.numpy as jnp
from jax import lax
from jax.experimental import pallas as pl
from jax.experimental.pallas import tpu as pltpu
from jax.sharding import PartitionSpec as P


F32, BF16, I32 = jnp.float32, jnp.bfloat16, jnp.int32
HOT_ROWS = 1024
COLD_ROWS = 1024
STEP = 128
GATHER = STEP
UP_COLS = 1920
DOWN_COLS = 768
VMEM_LIMIT = 60 << 20
ANY = pl.BlockSpec(memory_space=pl.ANY)


def params(n):
    return pltpu.CompilerParams(dimension_semantics=("arbitrary",) * n, vmem_limit_bytes=VMEM_LIMIT)


def gelu(v):
    return jax.nn.gelu(v, approximate=True).astype(BF16)


def prep_body(cap, scal, idx_ref, base_ref, pos_ref, cnt_ref):
    hot, own, r1, r2 = scal[0], scal[1], scal[2], scal[3]
    w = 256
    tri = (lax.broadcasted_iota(I32, (w, w), 0) <= lax.broadcasted_iota(I32, (w, w), 1)).astype(F32)
    base = ((base_ref[...] + STEP - 1) // STEP * STEP)[:, 0:1].astype(F32)
    carry = jnp.zeros((8, 1), F32)
    pos_ref[...] = jnp.full(pos_ref.shape, -1, I32)
    for b in range(idx_ref.shape[1] // w):
        cols = pl.ds(b * w, w)
        c0, c1 = idx_ref[0:1, cols], idx_ref[1:2, cols]
        cold = jnp.where(c0 == hot, c1, c0)
        loc = jnp.where(cold == own, 0, jnp.where(cold == own + 1, 1, jnp.where(cold == r1, 2, jnp.where(cold == r2, 3, -1))))
        mine = (lax.broadcasted_iota(I32, (8, w), 0) == loc).astype(F32)
        upto = jnp.dot(mine, tri, preferred_element_type=F32) + carry
        rank = jnp.sum(mine * (upto + base - 1.0), axis=0, keepdims=True).astype(I32)
        pos_ref[0:1, cols] = jnp.where(loc >= 0, loc * cap + rank, -1)
        carry = upto[:, w - 1:w]
    cnt_ref[...] = jnp.broadcast_to(carry, (8, 128)).astype(I32)


def prep(scal, idx8, base, cap):
    vmem = pl.BlockSpec(memory_space=pltpu.VMEM)
    return pl.pallas_call(
        functools.partial(prep_body, cap),
        out_shape=(jax.ShapeDtypeStruct(idx8.shape, I32), jax.ShapeDtypeStruct((8, 128), I32)),
        in_specs=[pl.BlockSpec(memory_space=pltpu.SMEM), vmem, vmem],
        out_specs=(vmem, vmem),
    )(scal, idx8, base)


def gather_body(n_parts, blk, pos_ref, *refs):
    parts, out_ref = refs[:n_parts], refs[-1]
    i = pl.program_id(0)

    @pl.when(i < blk[pl.num_programs(0)])
    def _():
        total, start = None, 0
        for part in parts:
            width = part.shape[0]
            slot = blk[i] * GATHER + lax.broadcasted_iota(I32, (GATHER, width), 0)
            pick = (pos_ref[0:1, start:start + width] == slot).astype(F32).astype(BF16)
            term = jnp.dot(pick, part[...], preferred_element_type=F32)
            total = term if total is None else total + term
            start += width
        out_ref[...] = total.astype(BF16)


def gather(blk, pos, parts, slots, prev, dep):
    d = parts[0].shape[1]
    alias = prev is not None
    return pl.pallas_call(
        functools.partial(gather_body, len(parts)),
        out_shape=jax.ShapeDtypeStruct((slots, d), BF16),
        grid_spec=pltpu.PrefetchScalarGridSpec(
            num_scalar_prefetch=1, grid=(blk.shape[0] - 1,),
            in_specs=[pl.BlockSpec(pos.shape, lambda i, b: (0, 0))]
            + [pl.BlockSpec(p.shape, lambda i, b: (0, 0)) for p in parts] + [ANY] * (1 + alias),
            out_specs=pl.BlockSpec((GATHER, d), lambda i, b: (b[i], 0))),
        input_output_aliases={3 + len(parts): 0} if alias else {},
        compiler_params=params(1),
    )(blk, pos, *parts, dep, *([prev] if alias else []))


def ffn_body(n_sets, rb, hot, x_ref, *refs):
    metas, ups, downs = refs[:n_sets], refs[n_sets:2 * n_sets], refs[2 * n_sets:3 * n_sets]
    out_ref, hid_ref = refs[-2:]
    d, ff = ups[0].shape[1:]

    def for_rows(meta, i, run):
        if hot:
            lax.fori_loop(0, rb // 512, lambda r, c: (run(r * 512, 512), c)[1], 0)
            return
        steps = meta[2, i]
        lax.fori_loop(0, steps // 4, lambda r, c: (run(r * 512, 512), c)[1], 0)

        @pl.when(steps % 4 >= 2)
        def _():
            run(steps // 4 * 512, 256)

        @pl.when(steps % 2 == 1)
        def _():
            run((steps - 1) * STEP, STEP)

    for meta, up, down in zip(metas, ups, downs):
        n = meta[3, 0]

        def up_step(step, x, w, h, meta=meta):
            def run(r, m):
                rows = pl.ds(pl.multiple_of(r, m), m)
                h[rows, :] = gelu(jnp.dot(x[rows, :], w[0], preferred_element_type=F32))

            for_rows(meta, step.index[0], run)

        def down_step(step, h, w, o, meta=meta):
            if not hot:
                o[...] = jnp.zeros_like(o)

            def run(r, m):
                rows = pl.ds(pl.multiple_of(r, m), m)
                o[rows, :] = jnp.dot(h[rows, :], w[0], preferred_element_type=F32).astype(BF16)

            for_rows(meta, step.index[0], run)

        @pl.when(n > 0)
        def _(meta=meta, up=up, down=down, up_step=up_step, down_step=down_step, n=n):
            pltpu.emit_pipeline(
                up_step, grid=(n, ff // UP_COLS),
                in_specs=[pl.BlockSpec((rb, d), lambda i, f: (meta[0, i], 0)),
                          pl.BlockSpec((1, d, UP_COLS), lambda i, f: (meta[1, i], 0, f))],
                out_specs=[pl.BlockSpec((rb, UP_COLS), lambda i, f: (i, f))],
                _explicit_indices=True,
            )(x_ref, up, hid_ref)
            pltpu.emit_pipeline(
                down_step, grid=(n, d // DOWN_COLS),
                in_specs=[pl.BlockSpec((rb, ff), lambda i, c: (i, 0)),
                          pl.BlockSpec((1, ff, DOWN_COLS), lambda i, c: (meta[1, i], 0, c))],
                out_specs=[pl.BlockSpec((rb, DOWN_COLS), lambda i, c: (meta[0, i], c))],
                _explicit_indices=True,
            )(hid_ref, down, out_ref)


def ffn(sets, x, dep, prev, rb, hot, out_rows):
    n = len(sets)
    metas, ups, downs = zip(*sets)
    d, ff = ups[0].shape[1:]
    max_items = max(m.shape[1] for m in metas)
    alias = prev is not None
    out, _ = pl.pallas_call(
        functools.partial(ffn_body, n, rb, hot),
        out_shape=(jax.ShapeDtypeStruct((out_rows, d), BF16), jax.ShapeDtypeStruct((max_items * rb, ff), BF16)),
        in_specs=[ANY] + [pl.BlockSpec(memory_space=pltpu.SMEM)] * n + [ANY] * (2 * n + 1 + alias),
        out_specs=(ANY, ANY),
        input_output_aliases={3 * n + 2: 0} if alias else {},
        compiler_params=pltpu.CompilerParams(vmem_limit_bytes=VMEM_LIMIT),
    )(x, *metas, *ups, *downs, dep, *([prev] if alias else []))
    return out


def after_body(value, dep, out):
    out[0] = value[0]


def after(value, dep):
    smem = pl.BlockSpec(memory_space=pltpu.SMEM)
    return pl.pallas_call(after_body, out_shape=jax.ShapeDtypeStruct((1,), I32), in_specs=[smem, ANY], out_specs=smem)(
        value.astype(I32)[None], dep)[0]


def join_body(local, blk, scal, pos_ref, gate_ref, hot_ref, cold_ref, out_ref, acc):
    k = pl.program_id(1)
    t = pos_ref.shape[0]

    @pl.when(k == 0)
    def _():
        acc[...] = jnp.zeros_like(acc)

    @pl.when(k < blk[pl.num_programs(1)])
    def _():
        slot = blk[k] * GATHER + lax.broadcasted_iota(I32, (t, GATHER), 1)
        pick = (pos_ref[:, 0:1] == slot).astype(F32).astype(BF16)
        acc[...] += jnp.dot(pick, cold_ref[...], preferred_element_type=F32)

    @pl.when(k == pl.num_programs(1) - 1)
    def _():
        for r in range(0, t, 256):
            rows = slice(r, r + 256)
            here = jnp.broadcast_to(pos_ref[rows, 0:1], (256, acc.shape[1])) >= 0
            g_hot, g_cold = gate_ref[rows, 0:1], gate_ref[rows, 1:2]
            o_hot, o_cold = hot_ref[rows, :].astype(F32), acc[rows, :]

            @pl.when(scal[0] == 1)
            def _():
                if local:
                    out_ref[rows, :] = g_hot * o_hot + jnp.where(here, g_cold * o_cold, 0.0)
                else:
                    out_ref[rows, :] = jnp.where(here, g_hot * o_hot + g_cold * o_cold, o_hot).astype(BF16)

            @pl.when(scal[0] == 0)
            def _():
                if local:
                    out_ref[rows, :] = jnp.where(here, g_cold * o_cold, 0.0)
                else:
                    out_ref[rows, :] = o_cold.astype(BF16)


def join(blk, scal, pos_col, gates, o_hot, o_cold, local, first, rows):
    d = o_hot.shape[1]
    tb = 1024
    return pl.pallas_call(
        functools.partial(join_body, local),
        out_shape=jax.ShapeDtypeStruct((rows, d), F32 if local else BF16),
        grid_spec=pltpu.PrefetchScalarGridSpec(
            num_scalar_prefetch=2, grid=(rows // tb, blk.shape[0] - 1),
            in_specs=[pl.BlockSpec((tb, 1), lambda i, k, b, s: (i + first, 0)),
                      pl.BlockSpec((tb, 2), lambda i, k, b, s: (i + first, 0)),
                      pl.BlockSpec((tb, d), lambda i, k, b, s: (i, 0)),
                      pl.BlockSpec((GATHER, d), lambda i, k, b, s: (b[k], 0))],
            out_specs=pl.BlockSpec((tb, d), lambda i, k, b, s: (i, 0)),
            scratch_shapes=[pltpu.VMEM((tb, d), F32)]),
        compiler_params=params(2),
    )(blk, scal, pos_col, gates, o_hot, o_cold)


def final_body(part_ref, gate_ref, back_ref, prev_ref, out_ref):
    out_ref[...] = (part_ref[...] + gate_ref[...] * back_ref[...].astype(F32)).astype(BF16)


def final(part, gate, back, prev, half):
    rows, d = part.shape
    tb = 256
    n = rows // 2 // tb
    return pl.pallas_call(
        final_body,
        out_shape=jax.ShapeDtypeStruct((rows, d), BF16),
        grid=(n,),
        in_specs=[pl.BlockSpec((tb, d), lambda i: (i + half * n, 0)), pl.BlockSpec((tb, 1), lambda i: (i + half * n, 0)),
                  pl.BlockSpec((tb, d), lambda i: (i, 0)), ANY],
        out_specs=pl.BlockSpec((tb, d), lambda i: (i + half * n, 0)),
        input_output_aliases={3: 0} if prev is not None else {},
        compiler_params=params(1),
    )(part, gate, back, prev if prev is not None else back)


def cold_items(steps, locs, cap):
    per = COLD_ROWS // STEP
    n = [(steps[l] + per - 1) // per for l in locs]
    i = jnp.arange(cap // COLD_ROWS + len(locs), dtype=I32)
    block, exp, left = locs[0] * (cap // COLD_ROWS) + i, jnp.zeros_like(i), steps[locs[0]] - i * per
    if len(locs) == 2:
        second = i >= n[0]
        j = i - n[0]
        block = jnp.where(second, locs[1] * (cap // COLD_ROWS) + j, block)
        exp = second.astype(I32)
        left = jnp.where(second, steps[locs[1]] - j * per, left)
    return jnp.stack([jnp.clip(block, 0, 4 * cap // COLD_ROWS - 1), exp, jnp.clip(left, 1, per), jnp.full_like(i, sum(n))])


def gather_blocks(n, first, cap, tokens):
    i = jnp.arange(tokens // GATHER + 4, dtype=I32)
    i = jnp.minimum(i, sum(n) - 1)
    blk, start = jnp.zeros_like(i), 0
    for l in range(4):
        blk = jnp.where(i >= start, l * (cap // GATHER) + first[l] + i - start, blk)
        start = start + n[l]
    return jnp.concatenate([jnp.clip(blk, 0, 4 * cap // GATHER - 1), jnp.full((1,), start, I32)])


def solution(mesh):
    group = mesh.shape['expert']
    n_exp = 2 * group
    sib = [(i, i ^ 1) for i in range(group)]
    far = [(i, i ^ 2) for i in range(group)]

    def send(v, pairs):
        return lax.ppermute(v, 'expert', pairs)

    def layer(x, idx, gate, up, down):
        tokens, _ = x.shape
        half = tokens // 2
        cap = 2 * tokens
        me = lax.axis_index('expert')
        p_idx = send(idx, far)
        p_gate = send(gate, far)

        taken = [jnp.sum((idx == k).astype(I32)) == tokens for k in range(n_exp)]
        hot = sum(jnp.where(t, k, 0) for k, t in enumerate(taken)).astype(I32)
        owner = hot // 2
        sel = jnp.where(owner == me, hot % 2, 0)
        peer = me ^ 1
        p_sel = jnp.where(owner == peer, hot % 2, 0)
        ids = jnp.stack([hot, 2 * me, 2 * peer + p_sel, 2 * peer + 1 - p_sel]).astype(I32)
        hot_here = owner // 2 == me // 2
        flag = hot_here.astype(I32)[None]

        far1 = send(x[:half], far)
        far2 = send(x[half:], far)
        sel_1 = after(sel, idx)
        up1 = lax.dynamic_slice_in_dim(up, sel_1, 1, 0)
        down1 = lax.dynamic_slice_in_dim(down, after(sel_1, up1), 1, 0)
        other = after(1 - sel_1, down1)
        up1 = send(up1, sib)
        down1 = send(down1, sib)

        def rows8(i):
            return jnp.concatenate([i.T, jnp.full((6, tokens), -1, I32)], axis=0)

        pos_o, cnt_o = prep(ids, rows8(idx), jnp.zeros((8, 128), I32), cap)
        pos_p, cnt_p = prep(ids, rows8(p_idx), cnt_o, cap)
        n_o = [(cnt_o[l, 0] + STEP - 1) // STEP for l in range(4)]
        n_p = [(cnt_p[l, 0] + STEP - 1) // STEP for l in range(4)]
        n_all = [a + b for a, b in zip(n_o, n_p)]
        blk_o = gather_blocks(n_o, [0] * 4, cap, tokens)
        blk_p = gather_blocks(n_p, n_o, cap, tokens)
        col_o, col_p = pos_o[0][:, None], pos_p[0][:, None]

        rows_o = gather(blk_o, pos_o, (x,), 4 * cap, None, pos_o)
        up2 = send(lax.dynamic_slice_in_dim(up, other, 1, 0), sib)
        down2 = send(lax.dynamic_slice_in_dim(down, other, 1, 0), sib)

        def gates(i, g):
            first = i[:, 0:1] == hot
            return jnp.concatenate([jnp.where(first, g[:, 0:1], g[:, 1:2]), jnp.where(first, g[:, 1:2], g[:, 0:1])], axis=1)

        g_o, g_p = gates(idx, gate), gates(p_idx, p_gate)
        here = col_o >= 0
        g_back = jnp.where(hot_here, jnp.where(here, 0.0, g_o[:, 1:2]), jnp.where(here, g_o[:, 0:1], 1.0))
        own_hot, got_hot = (owner == me).astype(I32), (owner == peer).astype(I32)

        def run_hot(xs, first, n, sets, dep, prev):
            i = jnp.arange(n, dtype=I32)
            sets = [(jnp.stack([i + first, jnp.full_like(i, exp), i, jnp.full_like(i, n * on)]), u, dn) for exp, on, u, dn in sets]
            return ffn(sets, xs, dep, prev, HOT_ROWS, True, xs.shape[0])

        hot_own, hot_got = (hot % 2, own_hot, up, down), (0, got_hot, up1, down1)
        hot_o = run_hot(x, 0, 2, [hot_own], rows_o, None)
        hot_1 = run_hot(far1, 0, 1, [hot_own, hot_got], hot_o, None)
        hot_o = run_hot(x, 0, 1, [hot_got], hot_1, hot_o)
        rows = gather(blk_p, pos_p, (far1, far2), 4 * cap, rows_o, hot_o)
        sets = [(cold_items(n_all, (0, 1), cap), up, down), (cold_items(n_all, (2,), cap), up1, down1),
                (cold_items(n_all, (3,), cap), up2, down2)]
        cold = ffn(sets, rows, rows, None, COLD_ROWS, False, 4 * cap)
        out_1 = join(blk_p, flag, col_p, g_p, hot_1, cold, False, 0, half)
        back_1 = send(out_1, far)
        hot_2 = run_hot(far2, 0, 1, [hot_own, hot_got], out_1, None)
        out_2 = join(blk_p, flag, col_p, g_p, hot_2, cold, False, 1, half)
        back_2 = send(out_2, far)
        hot_o = run_hot(x, 1, 1, [hot_got], out_2, hot_o)
        part = join(blk_o, flag, col_o, g_o, hot_o, cold, True, 0, tokens)
        y = final(part, g_back, back_1, None, 0)
        return final(part, g_back, back_2, y, 1)

    tok_spec = P(('data', 'expert'), None)
    w_spec = P('expert', None, None)
    return jax.shard_map(layer, mesh=mesh, in_specs=(tok_spec, tok_spec, tok_spec, w_spec, w_spec), out_specs=tok_spec, check_vma=False)
```
